128 devices in a mesh: prompt: 16 (over z, x_lo, core), ctx: 8 (over x_hi, y).
Axes of the slice: x: 4 (x_hi: 2, x_lo: 2; x = x_hi * 2 + x_lo), y: 4, z: 4, core: 2. Of those that a mesh axis runs over, the one named last changes fastest.
Arguments:
- queries: bfloat16 [65536, 16, 128], P(('prompt', 'ctx')), may hold values from -8 to 8
- keys: bfloat16 [65536, 4, 128], P(('prompt', 'ctx')), may hold values from -8 to 8
- values: bfloat16 [65536, 4, 128], P(('prompt', 'ctx')), may hold values from -6 to 6
- spans: int32 [16, 2], P('prompt'), may hold values from 1 to 3072, as said below
- partner: int32 [16], replicated, may hold values from 0 to 15, each once
Outputs:
- attended: bfloat16 [65536, 16, 128], P(('prompt', 'ctx'))
- decode_cache: bfloat16 [16, 2, 16, 8, 128, 128], P('ctx', None, 'prompt')
The draws below stay inside these ranges and needn't reach their ends.
Inputs may be any that keep to these rules, and one draw needn't show every extreme that they name: `spans`: column 0 counts the image tokens of a prompt, from 1024 to 2048, which come first; column 1 counts the text tokens after them, 1 or more; the two sum to at most 4096, and to exactly 4096 for at least one prompt.
All inputs are finite; a program needn't handle non-finite values.
Results may differ from the reference program's by a relative error of at most 0.0041.
Values may be sent and summed in bfloat16 or wider, within the bound.
A program may use at most 64 MiB of HBM per device.

```python
import math
import jax
import jax.numpy as jnp
from jax import lax

HEADS = 16
KVH = 4
HD = 128
SEQ = 4096
PROMPTS = 16
TOKENS = 65536
STRIPES = 4
BLOCKS = 8
ROWS_STRIPE = 128


def draw_queries(key, part):
    drawn = jnp.clip(jax.random.normal(jax.random.fold_in(key, 11), (TOKENS, HEADS, HD), jnp.float32), -4.0, 4.0)
    return drawn.astype(jnp.bfloat16)


def draw_keys(key, part):
    drawn = jnp.clip(jax.random.normal(jax.random.fold_in(key, 21), (TOKENS, KVH, HD), jnp.float32), -4.0, 4.0)
    return drawn.astype(jnp.bfloat16)


def draw_spans(key, part):
    image_count = jax.random.randint(jax.random.fold_in(key, 31), (PROMPTS,), SEQ // 4, SEQ // 2 + 1)
    text_count = jax.random.randint(jax.random.fold_in(key, 32), (PROMPTS,), 1, SEQ - image_count + 1)
    fullest = jax.random.randint(jax.random.fold_in(key, 33), (), 0, PROMPTS)
    shortest = (fullest + 1) % PROMPTS
    index_row = jnp.arange(PROMPTS)
    image_count = jnp.where(index_row == fullest, SEQ // 4, image_count)
    text_count = jnp.where(index_row == fullest, SEQ - SEQ // 4, text_count)
    text_count = jnp.where(index_row == shortest, 1, text_count)
    return jnp.stack([image_count, text_count], axis=1).astype(jnp.int32)


def levels(key, dims, split, smallest, top_value):
    def one(position, parts):
        draws = jax.random.uniform(jax.random.fold_in(jax.random.fold_in(key, 6), position), (parts,), jnp.float32, smallest / len(split), top_value / len(split))
        return jnp.repeat(jnp.exp(draws), dims[position] // parts).reshape((-1,) + (1,) * (len(dims) - position - 1))

    gain = one(*split[0])
    for cut in split[1:]:
        gain = gain * one(*cut)
    return gain


def scatter_about(stream_key, dims, scale, most, cuts=(), kind=jnp.bfloat16):
    values = scale * jax.random.normal(stream_key, dims, jnp.float32)
    if cuts:
        values = values * levels(stream_key, dims, cuts, -0.22, 0.18)
    return jnp.clip(values, -most, most).astype(kind)


def setup_inputs(seed: int = 0) -> dict:
    key_list = jax.random.split(jax.random.key(seed), 6)
    return {
        "queries": draw_queries(jax.random.fold_in(key_list[5], 71), 0),
        "keys": draw_keys(jax.random.fold_in(key_list[5], 71), 0),
        "values": scatter_about(key_list[2], (TOKENS, KVH, HD), 1.0, 6.0, ((0, 128),)),
        "spans": draw_spans(jax.random.fold_in(key_list[5], 71), 0),
        "partner": jax.random.permutation(key_list[4], PROMPTS).astype(jnp.int32),
    }


def attend_prompt(prompt_item):
    prompt_queries, prompt_keys, prompt_values, length = prompt_item
    qblock = math.gcd(SEQ, 512)
    block_count = SEQ // qblock
    members = HEADS // KVH
    grouped = prompt_queries.reshape(block_count, qblock, KVH, members, HD)
    keys_wide = prompt_keys.astype(jnp.float32)
    values_wide = prompt_values.astype(jnp.float32)
    key_pos = lax.iota(jnp.int32, SEQ)

    def one_block(block_item):
        query_block, block_index = block_item
        query_pos = block_index * qblock + lax.iota(jnp.int32, qblock)
        scores = jnp.einsum('qgmd,kgd->qgmk', query_block.astype(jnp.float32), keys_wide) * (1.0 / math.sqrt(HD))
        allowed = ((key_pos[None, :] <= query_pos[:, None]) & (key_pos[None, :] < length))[:, None, None, :]
        scores = jnp.where(allowed, scores, -1e+30)
        row_peak = lax.optimization_barrier(jnp.max(scores, axis=-1, keepdims=True))
        weights = jnp.where(allowed, jnp.exp(scores - row_peak), 0.0)
        rounded = lax.optimization_barrier(weights.astype(jnp.bfloat16)).astype(jnp.float32)
        mixture = jnp.einsum('qgmk,kgd->qgmd', rounded, values_wide) / lax.optimization_barrier(jnp.sum(weights, axis=-1))[..., None]
        mixture = jnp.where((query_pos < length)[:, None, None, None], mixture, 0.0)
        return mixture.reshape(qblock, HEADS, HD).astype(jnp.bfloat16)
    finished = lax.map(one_block, (grouped, jnp.arange(block_count, dtype=jnp.int32)))
    return finished.reshape(SEQ, HEADS, HD)

def reference(queries, keys, values, spans, partner):
    lengths = spans[:, 0] + spans[:, 1]
    prompt_queries = queries.reshape(PROMPTS, SEQ, HEADS, HD)
    prompt_keys = keys.reshape(PROMPTS, SEQ, KVH, HD)
    prompt_values = values.reshape(PROMPTS, SEQ, KVH, HD)
    attended = lax.map(attend_prompt, (prompt_queries, prompt_keys, prompt_values, lengths))
    attended = attended.reshape(TOKENS, HEADS, HD)
    live_rows = (lax.iota(jnp.int32, SEQ)[None, :] < lengths[:, None])[:, :, None, None]
    paired = jnp.stack([jnp.where(live_rows, prompt_keys, jnp.zeros_like(prompt_keys)), jnp.where(live_rows, prompt_values, jnp.zeros_like(prompt_values))], axis=1)
    paired = jnp.take(paired, partner.astype(jnp.int32), axis=0)
    paired = paired.reshape(PROMPTS, 2, BLOCKS, ROWS_STRIPE, STRIPES, KVH, HD)
    decode_cache = paired.transpose(0, 1, 4, 5, 2, 3, 6).reshape(PROMPTS, 2, STRIPES * KVH, BLOCKS, ROWS_STRIPE, HD)
    return (attended, decode_cache)
```

```python
import functools
import math

import jax
import jax.numpy as jnp
from jax import lax
from jax.experimental import pallas as pl
from jax.experimental.pallas import tpu as pltpu
from jax.sharding import PartitionSpec as P


def sent_together(arrays, axis, split_dim, concat_dim, along):
    widths = [a.shape[along] for a in arrays]
    both = jnp.concatenate(arrays, axis=along)
    whole = lax.all_to_all(both, axis, split_axis=split_dim, concat_axis=concat_dim, tiled=True)
    return tuple(jnp.split(whole, [sum(widths[:k]) for k in range(1, len(widths))], axis=along))


LOG2E = 1.4426950408889634

def head_block(kb, vt1, qt, m, acc, c, mask=None):
    s = lax.dot_general(kb, qt, (((1,), (0,)), ((), ())), preferred_element_type=jnp.float32)
    if mask is not None:
        s = jnp.where(mask, s, -1e30)
    top = jnp.max(s, axis=0, keepdims=True)
    if m is not None:
        new = jnp.maximum(m, top)
    else:
        new = top
    p = jnp.exp2(s * c - new * c).astype(jnp.bfloat16)
    o = lax.dot_general(vt1, p, (((1,), (0,)), ((), ())), preferred_element_type=jnp.float32)
    if m is not None:
        o = acc * jnp.exp2((m - new) * c) + o
    return new, o

def flash_kernel(heads, tq, len_ref, q_ref, k_ref, v_ref, o_ref, vt, qt, ms, acc):
    i = pl.program_id(0)
    d = k_ref.shape[1]
    c = LOG2E / math.sqrt(d)
    nblk = k_ref.shape[0] // tq
    @pl.when(i == 0)
    def _():
        for j in range(nblk):
            vt[j, 0:d, :] = v_ref[j * tq:(j + 1) * tq, :].T
            vt[j, d:, :] = jnp.ones((16, tq), jnp.bfloat16)
    for h in range(heads):
        qt[h] = q_ref[h].T
    base = pl.multiple_of(i * tq, tq)
    kd = k_ref[pl.ds(base, tq), :]
    rows = lax.broadcasted_iota(jnp.int32, (tq, tq), 0)
    cols = lax.broadcasted_iota(jnp.int32, (tq, tq), 1)
    n = len_ref[0]
    for h in range(heads):
        m, o = head_block(kd, vt[i], qt[h], None, None, c, (rows <= cols) & (base + rows < n) | (rows == 0))
        ms[h] = m
        acc[h] = o
    def step(j, carry):
        kb = k_ref[pl.ds(pl.multiple_of(j * tq, tq), tq), :]
        vb = vt[j]
        for h in range(heads):
            m, o = head_block(kb, vb, qt[h], ms[h], acc[h], c)
            ms[h] = m
            acc[h] = o
        return carry
    lax.fori_loop(0, jnp.where(base < n, i, 0), step, 0)
    live = base + lax.broadcasted_iota(jnp.int32, (tq, 1), 0) < n
    for h in range(heads):
        o = acc[h]
        r = (o[0:d, :] / o[d:d + 1, :]).T
        o_ref[h] = jnp.where(live, r, 0.0).astype(jnp.bfloat16)

def flash(length, q, k, v, tq=512):
    heads, seq, d = q.shape
    return pl.pallas_call(
        functools.partial(flash_kernel, heads, tq),
        out_shape=jax.ShapeDtypeStruct(q.shape, jnp.bfloat16),
        grid_spec=pltpu.PrefetchScalarGridSpec(
            num_scalar_prefetch=1, grid=(seq // tq,),
            in_specs=[pl.BlockSpec((heads, tq, d), lambda i, n: (0, i, 0)),
                      pl.BlockSpec((seq, d), lambda i, n: (0, 0)),
                      pl.BlockSpec((seq, d), lambda i, n: (0, 0))],
            out_specs=pl.BlockSpec((heads, tq, d), lambda i, n: (0, i, 0)),
            scratch_shapes=[pltpu.VMEM((seq // tq, d + 16, tq), jnp.bfloat16),
                            pltpu.VMEM((heads, d, tq), jnp.bfloat16),
                            pltpu.VMEM((heads, 1, tq), jnp.float32),
                            pltpu.VMEM((heads, d + 16, tq), jnp.float32)]),
        compiler_params=pltpu.CompilerParams(dimension_semantics=("arbitrary",)),
        cost_estimate=pl.CostEstimate(flops=4 * heads * seq * seq * d // 2, bytes_accessed=8 << 20, transcendentals=heads * seq * seq // 2),
    )(length, q, k, v)

def per_device(queries, keys, values, spans, partner):
    tok_rows, head_count, head_width = queries.shape
    kv_heads = keys.shape[1]
    blocks = lax.axis_size("ctx")
    ctx_index = lax.axis_index("ctx")
    length = spans[0, 0] + spans[0, 1]
    stripes = lax.axis_size("prompt") // kv_heads
    live_rows = (ctx_index * tok_rows + lax.iota(jnp.int32, tok_rows) < length)[:, None, None]
    handoff = jnp.stack(
        [
            jnp.where(live_rows, keys, jnp.zeros_like(keys)),
            jnp.where(live_rows, values, jnp.zeros_like(values)),
        ]
    )
    handoff = handoff.reshape(1, 2, tok_rows // stripes, stripes * kv_heads, head_width)
    handoff = lax.all_to_all(handoff, "prompt", split_axis=3, concat_axis=0, tiled=True)
    handoff = jnp.take(handoff, partner, axis=0)
    handoff = handoff.reshape(handoff.shape[0], 2, 1, 1, tok_rows // stripes, head_width)
    handoff = lax.all_to_all(handoff, "ctx", split_axis=0, concat_axis=3, tiled=True)
    head_share = head_count // blocks
    copies = max(1, blocks // kv_heads)
    own_kv = kv_heads * copies // blocks
    query_split = queries.reshape(tok_rows, blocks, head_share, head_width)
    key_split = jnp.repeat(keys, copies, axis=1).reshape(tok_rows, blocks, own_kv, head_width)
    value_split = jnp.repeat(values, copies, axis=1).reshape(tok_rows, blocks, own_kv, head_width)
    query_all, key_all, value_all = sent_together(
        (query_split, key_split, value_split), "ctx", 1, 0, 2
    )
    sequence = blocks * tok_rows
    key_all = key_all.reshape(sequence, own_kv, head_width)
    value_all = value_all.reshape(sequence, own_kv, head_width)
    query_heads = query_all.reshape(sequence, head_share, head_width).transpose(1, 0, 2)
    finished = flash(length[None], query_heads, key_all[:, 0], value_all[:, 0])
    finished = finished.transpose(1, 0, 2).reshape(blocks, tok_rows, head_share, head_width)
    attended = lax.all_to_all(finished, "ctx", split_axis=0, concat_axis=2, tiled=True).reshape(
        tok_rows, head_count, head_width
    )
    return (attended, handoff)


def solution(mesh):
    placed = (
        P(("prompt", "ctx"), None, None),
        P(("prompt", "ctx"), None, None),
        P(("prompt", "ctx"), None, None),
        P("prompt", None),
        P(),
    )
    return jax.shard_map(
        per_device,
        mesh=mesh,
        in_specs=placed,
        out_specs=(P(("prompt", "ctx"), None, None), P("ctx", None, "prompt", None, None, None)),
        check_vma=False,
    )
```

```python
import functools
import math

import jax
import jax.numpy as jnp
from jax import lax
from jax.experimental import pallas as pl
from jax.experimental.pallas import tpu as pltpu
from jax.sharding import PartitionSpec as P

LOG2E = 1.4426950408889634
MESH = pl.DeviceIdType.MESH
ROUNDS = 10
CROSS = 8
DOT = (((1,), (0,)), ((), ()))


def fused_kernel(
    len_ref, partner_ref, q_ref, k_ref, v_ref, o_ref, cache_ref,
    own, inbox, relay, qt, peak, acc, score_a, score_b, spread, gathered, chosen, wide,
    link_send, link_recv, relay_recv, spread_send, spread_recv, hand_send, hand_recv,
):
    heads, rows, width = q_ref.shape
    groups = k_ref.shape[0]
    members = heads // groups
    tiles = rows // width
    scale = LOG2E / math.sqrt(width)
    scores = (score_a, score_b)

    prompts, blocks = lax.axis_size("prompt"), lax.axis_size("ctx")
    p, c = lax.axis_index("prompt"), lax.axis_index("ctx")
    ring = blocks // 2
    half, y = c // ring, c % ring
    flipped = p + 2 - 4 * ((p // 2) % 2)
    ahead = (p, half * ring + (y + 1) % ring)
    behind = (p, half * ring + (y + ring - 1) % ring)
    beside = (flipped, c)
    across = (flipped, (1 - half) * ring + y)
    length = len_ref[0]

    barrier = pltpu.get_barrier_semaphore()

    def greet_prompt(k, carry):
        pl.semaphore_signal(barrier, inc=1, device_id=((p + k) % prompts, c), device_id_type=MESH)
        return carry

    def greet_ctx(k, carry):
        pl.semaphore_signal(barrier, inc=1, device_id=(p, (c + k) % blocks), device_id_type=MESH)
        return carry

    lax.fori_loop(1, prompts, greet_prompt, 0)
    lax.fori_loop(1, blocks, greet_ctx, 0)
    pl.semaphore_signal(barrier, inc=1, device_id=across, device_id_type=MESH)

    for g in range(groups):
        own[g, 0:rows, :] = k_ref[g]
        for t in range(tiles):
            own[g, rows + t * width : rows + (t + 1) * width, :] = v_ref[
                g, t * width : (t + 1) * width, :
            ].T
    pl.semaphore_wait(barrier, prompts + blocks - 1)

    def put(src, dst, lane, i, recv, target):
        return pltpu.make_async_remote_copy(
            src_ref=src, dst_ref=dst, send_sem=link_send.at[lane, i], recv_sem=recv,
            device_id=target, device_id_type=MESH,
        )

    def send_ahead(i):
        @pl.when(i < 4)
        def _():
            put(own.at[i], inbox.at[0, i], 0, i, link_recv.at[0, i], ahead).start()

        @pl.when((i >= 4) & (i < 8))
        def _():
            put(inbox.at[0, i - 4], inbox.at[0, i], 0, i, link_recv.at[0, i], ahead).start()

        @pl.when((i >= 8) & (i < ROUNDS))
        def _():
            put(inbox.at[2, i - 3], inbox.at[0, i], 0, i, link_recv.at[0, i], ahead).start()

    def send_behind(i):
        @pl.when(i < 4)
        def _():
            put(own.at[i], inbox.at[1, i], 1, i, link_recv.at[1, i], behind).start()

        @pl.when((i >= 4) & (i < 8))
        def _():
            put(inbox.at[2, i - 3], inbox.at[1, i], 1, i, link_recv.at[1, i], behind).start()

        @pl.when((i >= 8) & (i < ROUNDS))
        def _():
            put(inbox.at[1, i - 4], inbox.at[1, i], 1, i, link_recv.at[1, i], behind).start()

    def send_beside(i):
        @pl.when(i < 4)
        def _():
            put(own.at[i], relay.at[i], 2, i, relay_recv.at[i], beside).start()

        @pl.when((i >= 4) & (i < CROSS))
        def _():
            put(inbox.at[0, (i - 2) % 4], relay.at[i], 2, i, relay_recv.at[i], beside).start()

    def send_across(i):
        put(relay.at[i], inbox.at[2, i + 1], 3, i, link_recv.at[2, i + 1], across).start()

    for i in range(2):
        send_ahead(jnp.int32(i))
        send_behind(jnp.int32(i))
        send_beside(jnp.int32(i))

    position = c * rows + lax.broadcasted_iota(jnp.int32, (rows, width), 0)
    stripes = spread.shape[0] // groups
    stripe_rows = rows // stripes
    for part, ref in enumerate((k_ref, v_ref)):
        for g in range(groups):
            wide[...] = jnp.where(position < length, ref[g].astype(jnp.float32), 0.0)
            for st in range(stripes):
                spread[st * groups + g, part] = wide[pl.ds(st, stripe_rows, stride=stripes), :].astype(jnp.bfloat16)

    def spread_copy(s):
        return pltpu.make_async_remote_copy(
            src_ref=spread.at[s], dst_ref=gathered.at[p], send_sem=spread_send.at[s],
            recv_sem=spread_recv.at[p], device_id=(s, c), device_id_type=MESH,
        )

    def spread_start(k, carry):
        spread_copy((p + k) % prompts).start()
        return carry

    gathered[p] = spread[p]
    lax.fori_loop(1, prompts, spread_start, 0)

    def turn(n, carry):
        qt[n] = q_ref[n].T
        peak[n] = jnp.full((1, rows), -1e30, jnp.float32)
        acc[n] = jnp.zeros(acc.shape[1:], jnp.float32)
        return carry

    lax.fori_loop(0, heads, turn, 0)

    def score(chunk, g, m):
        return lax.dot_general(
            chunk[0:rows, :], qt[g * members + m], DOT, preferred_element_type=jnp.float32
        )

    def fold(chunk, g, m, s, mask):
        n = g * members + m
        if mask is not None:
            s = jnp.where(mask, s, -1e30)
        before = peak[n]
        top = jnp.maximum(before, jnp.max(s, axis=0, keepdims=True))
        weight = jnp.exp2(s * scale - top * scale).astype(jnp.bfloat16)
        turned = jnp.concatenate(
            [chunk[rows + t * width : rows + (t + 1) * width, :] for t in range(tiles)], axis=1
        )
        turned = jnp.concatenate([turned, jnp.ones((acc.shape[1] - width, rows), jnp.bfloat16)], axis=0)
        mixed = lax.dot_general(turned, weight, DOT, preferred_element_type=jnp.float32)
        acc[n] = acc[n] * jnp.exp2((before - top) * scale) + mixed
        peak[n] = top

    def run(units, mask=None):
        chunk, g, m = units[0]
        scores[0][...] = score(chunk, g, m)
        for i, (chunk, g, m) in enumerate(units):
            if i + 1 < len(units):
                scores[(i + 1) % 2][...] = score(*units[i + 1])
            fold(chunk, g, m, scores[i % 2][...], mask)

    key_row = lax.broadcasted_iota(jnp.int32, (rows, rows), 0)
    query_row = lax.broadcasted_iota(jnp.int32, (rows, rows), 1)

    def diagonal(g, carry):
        mask = (key_row <= query_row) & ((c * rows + key_row < length) | (key_row == 0))
        run([(own.at[g], g, m) for m in range(members)], mask)
        return carry

    lax.fori_loop(0, groups, diagonal, 0)

    def lane_block(lane, i):
        near, far = half * ring, (1 - half) * ring
        ahead_block = jnp.where(
            i < 4, near + (y + ring - 1) % ring, jnp.where(i < 8, near + (y + 2) % ring, far + (y + 2) % ring)
        )
        behind_block = jnp.where(
            i < 4, near + (y + 1) % ring, jnp.where(i < 8, far + (y + 1) % ring, far + (y + 2) % ring)
        )
        across_block = jnp.where(i < 5, far + y, far + (y + ring - 1) % ring)
        block = jnp.where(lane == 0, ahead_block, jnp.where(lane == 1, behind_block, across_block))
        ahead_head = jnp.where(i < 8, i % 4, i - 6)
        across_head = jnp.where(i < 5, (i + 3) % 4, (i + 1) % 4)
        head = jnp.where(lane == 0, ahead_head, jnp.where(lane == 1, i % 4, across_head))
        return block, head

    def arrived(lane, i):
        put(inbox.at[lane, i], inbox.at[lane, i], lane, i, link_recv.at[lane, i], ahead).wait_recv()

    def hand_copy(k):
        target = (c + k) % blocks
        return pltpu.make_async_remote_copy(
            src_ref=chosen.at[pl.ds(2 * target, 2)], dst_ref=cache_ref.at[:, :, 0, c],
            send_sem=hand_send.at[target], recv_sem=hand_recv.at[c],
            device_id=(p, target), device_id_type=MESH,
        )

    def round_trip(i, carry):
        arrived(0, i)
        send_ahead(i + 2)
        send_beside(i + 2)

        @pl.when(i < CROSS)
        def _():
            put(relay.at[i], relay.at[i], 2, i, relay_recv.at[i], beside).wait_recv()
            send_across(i)

        arrived(1, i)
        send_behind(i + 2)

        crossing = (i >= 1) & (i <= CROSS)

        @pl.when(crossing)
        def _():
            arrived(2, i)

        @pl.when(i == CROSS)
        def _():
            def collect(k, inner):
                source = (p + k) % prompts
                pltpu.make_async_remote_copy(
                    src_ref=spread.at[source], dst_ref=gathered.at[source], send_sem=spread_send.at[source],
                    recv_sem=spread_recv.at[source], device_id=(source, c), device_id_type=MESH,
                ).wait_recv()
                return inner

            lax.fori_loop(1, prompts, collect, 0)
            for b in range(chosen.shape[0]):
                chosen[b] = gathered[partner_ref[b]]

            cache_ref[:, :, 0, c] = chosen[pl.ds(2 * c, 2)]

            def hand_start(k, inner):
                hand_copy(k).start()
                return inner

            lax.fori_loop(1, blocks, hand_start, 0)

        places = [lane_block(lane, i) for lane in range(3)]
        every = crossing & (places[0][0] < c) & (places[1][0] < c) & (places[2][0] < c)

        @pl.when(every)
        def _():
            run([(inbox.at[lane, i], places[lane][1], m) for lane in range(3) for m in range(members)])

        @pl.when(jnp.logical_not(every))
        def _():
            def one(lane, inner):
                block, g = lane_block(lane, i)

                @pl.when((block < c) & ((lane < 2) | crossing))
                def _():
                    run([(inbox.at[lane, i], g, m) for m in range(members)])

                return inner

            lax.fori_loop(0, 3, one, 0)

        return carry

    lax.fori_loop(0, ROUNDS, round_trip, 0)

    live = c * rows + lax.broadcasted_iota(jnp.int32, (rows, width), 0) < length

    def finish(n, carry):
        total = acc[n]
        mixture = (total[0:width] / total[width : width + 1]).T
        o_ref[n] = jnp.where(live, mixture, 0.0).astype(jnp.bfloat16)
        return carry

    lax.fori_loop(0, heads, finish, 0)

    def sent(i, carry):
        for lane in range(2):
            put(inbox.at[lane, i], inbox.at[lane, i], lane, i, link_recv.at[lane, i], ahead).wait_send()

        @pl.when(i < CROSS)
        def _():
            for lane in range(2, 4):
                put(relay.at[i], relay.at[i], lane, i, relay_recv.at[i], beside).wait_send()

        return carry

    lax.fori_loop(0, ROUNDS, sent, 0)

    def spread_done(k, carry):
        spread_copy((p + k) % prompts).wait_send()
        return carry

    lax.fori_loop(1, prompts, spread_done, 0)

    def hand_done(k, carry):
        hand_copy(k).wait_send()
        source = (c + k) % blocks
        pltpu.make_async_remote_copy(
            src_ref=chosen.at[pl.ds(2 * source, 2)], dst_ref=cache_ref.at[:, :, 0, source],
            send_sem=hand_send.at[source], recv_sem=hand_recv.at[source],
            device_id=(p, source), device_id_type=MESH,
        ).wait_recv()
        return carry

    lax.fori_loop(1, blocks, hand_done, 0)


def per_device(queries, keys, values, spans, partner):
    rows, heads, width = queries.shape
    groups = keys.shape[1]
    prompts, blocks = lax.axis_size("prompt"), lax.axis_size("ctx")
    stripe_rows = rows * groups // prompts
    vmem, smem = pl.BlockSpec(memory_space=pltpu.VMEM), pl.BlockSpec(memory_space=pltpu.SMEM)
    bf16, f32, dma = jnp.bfloat16, jnp.float32, pltpu.SemaphoreType.DMA
    piece = (2, stripe_rows, width)
    attended, cache = pl.pallas_call(
        fused_kernel,
        out_shape=(
            jax.ShapeDtypeStruct((heads, rows, width), bf16),
            jax.ShapeDtypeStruct((2, 2, 1, blocks, stripe_rows, width), bf16),
        ),
        in_specs=[smem, smem, vmem, vmem, vmem],
        out_specs=(vmem, vmem),
        scratch_shapes=[
            pltpu.VMEM((groups, 2 * rows, width), bf16),
            pltpu.VMEM((3, ROUNDS, 2 * rows, width), bf16),
            pltpu.VMEM((CROSS, 2 * rows, width), bf16),
            pltpu.VMEM((heads, width, rows), bf16),
            pltpu.VMEM((heads, 1, rows), f32),
            pltpu.VMEM((heads, width + 16, rows), f32),
            pltpu.VMEM((rows, rows), f32),
            pltpu.VMEM((rows, rows), f32),
            pltpu.VMEM((prompts,) + piece, bf16),
            pltpu.VMEM((prompts,) + piece, bf16),
            pltpu.VMEM((prompts,) + piece, bf16),
            pltpu.VMEM((rows, width), f32),
            dma((4, ROUNDS)),
            dma((3, ROUNDS)),
            dma((CROSS,)),
            dma((prompts,)),
            dma((prompts,)),
            dma((blocks,)),
            dma((blocks,)),
        ],
        compiler_params=pltpu.CompilerParams(
            collective_id=0, has_side_effects=True, vmem_limit_bytes=56 << 20
        ),
    )(
        spans[:, 0] + spans[:, 1],
        partner,
        queries.transpose(1, 0, 2),
        keys.transpose(1, 0, 2),
        values.transpose(1, 0, 2),
    )
    return attended.transpose(1, 0, 2), cache


def solution(mesh):
    placed = (
        P(("prompt", "ctx"), None, None),
        P(("prompt", "ctx"), None, None),
        P(("prompt", "ctx"), None, None),
        P("prompt", None),
        P(),
    )
    return jax.shard_map(
        per_device,
        mesh=mesh,
        in_specs=placed,
        out_specs=(P(("prompt", "ctx"), None, None), P("ctx", None, "prompt", None, None, None)),
        check_vma=False,
    )
```

```python
import functools
import math

import jax
import jax.numpy as jnp
from jax import lax
from jax.experimental import pallas as pl
from jax.experimental.pallas import tpu as pltpu
from jax.sharding import PartitionSpec as P

LOG2E = 1.4426950408889634
MESH = pl.DeviceIdType.MESH
ROUNDS = 10
CROSS = 8
HAND_ROUND = 8
DOT = (((1,), (0,)), ((), ()))


def fused_kernel(
    spans_ref, partner_ref, q_ref, k_ref, v_ref, o_ref, cache_ref,
    own, inbox, qt, peak, acc, score_a, score_b, spread, gathered, chosen, wide,
    link_send, link_recv, spread_send, spread_recv, hand_send, hand_recv,
):
    heads, rows, width = q_ref.shape
    groups = k_ref.shape[0]
    members = heads // groups
    tiles = rows // width
    scale = LOG2E / math.sqrt(width)
    scores = (score_a, score_b)

    prompts, blocks = lax.axis_size("prompt"), lax.axis_size("ctx")
    p, c = lax.axis_index("prompt"), lax.axis_index("ctx")
    ring = blocks // 2
    half, y = c // ring, c % ring
    ahead = (p, half * ring + (y + 1) % ring)
    behind = (p, half * ring + (y + ring - 1) % ring)
    across = (p, ring + y)
    length = spans_ref[0, 0] + spans_ref[0, 1]
    ahead_rounds = jnp.where(half == 0, 8, ROUNDS)
    behind_rounds = jnp.where(half == 0, 4, ROUNDS)

    barrier = pltpu.get_barrier_semaphore()

    def greet_prompt(k, carry):
        pl.semaphore_signal(barrier, inc=1, device_id=((p + k) % prompts, c), device_id_type=MESH)
        return carry

    def greet_ctx(k, carry):
        pl.semaphore_signal(barrier, inc=1, device_id=(p, (c + k) % blocks), device_id_type=MESH)
        return carry

    lax.fori_loop(1, prompts, greet_prompt, 0)
    lax.fori_loop(1, blocks, greet_ctx, 0)

    for g in range(groups):
        own[g, 0:rows, :] = k_ref[g]
        for t in range(tiles):
            own[g, rows + t * width : rows + (t + 1) * width, :] = v_ref[
                g, t * width : (t + 1) * width, :
            ].T
    pl.semaphore_wait(barrier, prompts + blocks - 2)

    def put(src, dst, lane, i, recv, target):
        return pltpu.make_async_remote_copy(
            src_ref=src, dst_ref=dst, send_sem=link_send.at[lane, i], recv_sem=recv,
            device_id=target, device_id_type=MESH,
        )

    def send_ahead(i):
        @pl.when(i < 4)
        def _():
            put(own.at[i], inbox.at[0, i], 0, i, link_recv.at[0, i], ahead).start()

        @pl.when((i >= 4) & (i < 8))
        def _():
            put(inbox.at[0, i - 4], inbox.at[0, i], 0, i, link_recv.at[0, i], ahead).start()

        @pl.when((i >= 8) & (i < ahead_rounds))
        def _():
            put(inbox.at[2, i - 3], inbox.at[0, i], 0, i, link_recv.at[0, i], ahead).start()

    def send_behind(i):
        @pl.when(i < 4)
        def _():
            put(own.at[i], inbox.at[1, i], 1, i, link_recv.at[1, i], behind).start()

        @pl.when((i >= 4) & (i < jnp.minimum(8, behind_rounds)))
        def _():
            put(inbox.at[2, i - 3], inbox.at[1, i], 1, i, link_recv.at[1, i], behind).start()

        @pl.when((i >= 8) & (i < behind_rounds))
        def _():
            put(inbox.at[1, i - 4], inbox.at[1, i], 1, i, link_recv.at[1, i], behind).start()

    def send_across(i):
        @pl.when((half == 0) & (i < 4))
        def _():
            put(own.at[i], inbox.at[2, i + 1], 2, i, link_recv.at[2, i + 1], across).start()

        @pl.when((half == 0) & (i >= 4) & (i < CROSS))
        def _():
            put(inbox.at[0, (i - 2) % 4], inbox.at[2, i + 1], 2, i, link_recv.at[2, i + 1], across).start()

    for i in range(2):
        send_ahead(jnp.int32(i))
        send_behind(jnp.int32(i))
        send_across(jnp.int32(i))

    position = c * rows + lax.broadcasted_iota(jnp.int32, (rows, width), 0)
    stripes = spread.shape[0] // groups
    stripe_rows = rows // stripes
    for part, ref in enumerate((k_ref, v_ref)):
        for g in range(groups):
            wide[...] = jnp.where(position < length, ref[g].astype(jnp.float32), 0.0)
            for st in range(stripes):
                spread[st * groups + g, part] = wide[pl.ds(st, stripe_rows, stride=stripes), :].astype(jnp.bfloat16)

    def spread_copy(s):
        return pltpu.make_async_remote_copy(
            src_ref=spread.at[s], dst_ref=gathered.at[p], send_sem=spread_send.at[s],
            recv_sem=spread_recv.at[p], device_id=(s, c), device_id_type=MESH,
        )

    def spread_start(k, carry):
        spread_copy((p + k) % prompts).start()
        return carry

    gathered[p] = spread[p]
    lax.fori_loop(1, prompts, spread_start, 0)

    def turn(n, carry):
        qt[n] = q_ref[n].T
        peak[n] = jnp.full((1, rows), -1e30, jnp.float32)
        acc[n] = jnp.zeros(acc.shape[1:], jnp.float32)
        return carry

    lax.fori_loop(0, heads, turn, 0)

    def score(chunk, g, m):
        return lax.dot_general(
            chunk[0:rows, :], qt[g * members + m], DOT, preferred_element_type=jnp.float32
        )

    def fold(chunk, g, m, s, mask):
        n = g * members + m
        if mask is not None:
            s = jnp.where(mask, s, -1e30)
        before = peak[n]
        top = jnp.maximum(before, jnp.max(s, axis=0, keepdims=True))
        weight = jnp.exp2(s * scale - top * scale).astype(jnp.bfloat16)
        turned = jnp.concatenate(
            [chunk[rows + t * width : rows + (t + 1) * width, :] for t in range(tiles)], axis=1
        )
        turned = jnp.concatenate([turned, jnp.ones((acc.shape[1] - width, rows), jnp.bfloat16)], axis=0)
        mixed = lax.dot_general(turned, weight, DOT, preferred_element_type=jnp.float32)
        acc[n] = acc[n] * jnp.exp2((before - top) * scale) + mixed
        peak[n] = top

    def run(units, mask=None):
        chunk, g, m = units[0]
        scores[0][...] = score(chunk, g, m)
        for i, (chunk, g, m) in enumerate(units):
            if i + 1 < len(units):
                scores[(i + 1) % 2][...] = score(*units[i + 1])
            fold(chunk, g, m, scores[i % 2][...], mask)

    key_row = lax.broadcasted_iota(jnp.int32, (rows, rows), 0)
    query_row = lax.broadcasted_iota(jnp.int32, (rows, rows), 1)

    def diagonal(g, carry):
        mask = (key_row <= query_row) & ((c * rows + key_row < length) | (key_row == 0))
        run([(own.at[g], g, m) for m in range(members)], mask)
        return carry

    lax.fori_loop(0, groups, diagonal, 0)

    def lane_block(lane, i):
        near, far = half * ring, (1 - half) * ring
        ahead_block = jnp.where(
            i < 4, near + (y + ring - 1) % ring, jnp.where(i < 8, near + (y + 2) % ring, far + (y + 2) % ring)
        )
        behind_block = jnp.where(
            i < 4, near + (y + 1) % ring, jnp.where(i < 8, far + (y + 1) % ring, far + (y + 2) % ring)
        )
        across_block = jnp.where(i < 5, far + y, far + (y + ring - 1) % ring)
        block = jnp.where(lane == 0, ahead_block, jnp.where(lane == 1, behind_block, across_block))
        ahead_head = jnp.where(i < 8, i % 4, i - 6)
        across_head = jnp.where(i < 5, (i + 3) % 4, (i + 1) % 4)
        head = jnp.where(lane == 0, ahead_head, jnp.where(lane == 1, i % 4, across_head))
        return block, head

    def arrived(lane, i):
        put(inbox.at[lane, i], inbox.at[lane, i], lane, i, link_recv.at[lane, i], ahead).wait_recv()

    def hand_copy(k):
        target = (c + k) % blocks
        return pltpu.make_async_remote_copy(
            src_ref=chosen.at[pl.ds(2 * target, 2)], dst_ref=cache_ref.at[:, :, 0, c],
            send_sem=hand_send.at[target], recv_sem=hand_recv.at[c],
            device_id=(p, target), device_id_type=MESH,
        )

    def round_trip(i, carry):
        @pl.when(i < ahead_rounds)
        def _():
            arrived(0, i)

        send_ahead(i + 2)
        send_across(i + 2)

        @pl.when(i < behind_rounds)
        def _():
            arrived(1, i)

        send_behind(i + 2)
        crossing = (half == 1) & (i >= 1) & (i <= CROSS)

        @pl.when(crossing)
        def _():
            arrived(2, i)

        @pl.when(i == HAND_ROUND)
        def _():
            def collect(k, inner):
                source = (p + k) % prompts
                pltpu.make_async_remote_copy(
                    src_ref=spread.at[source], dst_ref=gathered.at[source], send_sem=spread_send.at[source],
                    recv_sem=spread_recv.at[source], device_id=(source, c), device_id_type=MESH,
                ).wait_recv()
                return inner

            lax.fori_loop(1, prompts, collect, 0)
            for b in range(chosen.shape[0]):
                chosen[b] = gathered[partner_ref[b]]

            cache_ref[:, :, 0, c] = chosen[pl.ds(2 * c, 2)]

            def hand_start(k, inner):
                hand_copy(k).start()
                return inner

            lax.fori_loop(1, blocks, hand_start, 0)

        places = [lane_block(lane, i) for lane in range(3)]
        every = crossing & (places[0][0] < c) & (places[1][0] < c) & (places[2][0] < c)

        @pl.when(every)
        def _():
            run([(inbox.at[lane, i], places[lane][1], m) for lane in range(3) for m in range(members)])

        @pl.when(jnp.logical_not(every))
        def _():
            def one(lane, inner):
                block, g = lane_block(lane, i)

                @pl.when((block < c) & ((lane < 2) | crossing))
                def _():
                    run([(inbox.at[lane, i], g, m) for m in range(members)])

                return inner

            lax.fori_loop(0, 3, one, 0)

        return carry

    lax.fori_loop(0, ROUNDS, round_trip, 0)

    live = c * rows + lax.broadcasted_iota(jnp.int32, (rows, width), 0) < length

    def finish(n, carry):
        total = acc[n]
        mixture = (total[0:width] / total[width : width + 1]).T
        o_ref[n] = jnp.where(live, mixture, 0.0).astype(jnp.bfloat16)
        return carry

    lax.fori_loop(0, heads, finish, 0)

    def sent(i, carry):
        def left(lane, going):
            @pl.when(going)
            def _():
                put(inbox.at[0, i], inbox.at[0, i], lane, i, link_recv.at[0, i], ahead).wait_send()

        left(0, i < ahead_rounds)
        left(1, i < behind_rounds)
        left(2, (half == 0) & (i < CROSS))
        return carry

    lax.fori_loop(0, ROUNDS, sent, 0)

    def spread_done(k, carry):
        spread_copy((p + k) % prompts).wait_send()
        return carry

    lax.fori_loop(1, prompts, spread_done, 0)

    def hand_done(k, carry):
        hand_copy(k).wait_send()
        source = (c + k) % blocks
        pltpu.make_async_remote_copy(
            src_ref=chosen.at[pl.ds(2 * source, 2)], dst_ref=cache_ref.at[:, :, 0, source],
            send_sem=hand_send.at[source], recv_sem=hand_recv.at[source],
            device_id=(p, source), device_id_type=MESH,
        ).wait_recv()
        return carry

    lax.fori_loop(1, blocks, hand_done, 0)


def per_device(queries, keys, values, spans, partner):
    rows, heads, width = queries.shape
    groups = keys.shape[1]
    prompts, blocks = lax.axis_size("prompt"), lax.axis_size("ctx")
    stripe_rows = rows * groups // prompts
    vmem, smem = pl.BlockSpec(memory_space=pltpu.VMEM), pl.BlockSpec(memory_space=pltpu.SMEM)
    bf16, f32, dma = jnp.bfloat16, jnp.float32, pltpu.SemaphoreType.DMA
    piece = (2, stripe_rows, width)
    attended, cache = pl.pallas_call(
        fused_kernel,
        out_shape=(
            jax.ShapeDtypeStruct((heads, rows, width), bf16),
            jax.ShapeDtypeStruct((2, 2, 1, blocks, stripe_rows, width), bf16),
        ),
        in_specs=[smem, smem, vmem, vmem, vmem],
        out_specs=(vmem, vmem),
        scratch_shapes=[
            pltpu.VMEM((groups, 2 * rows, width), bf16),
            pltpu.VMEM((3, ROUNDS, 2 * rows, width), bf16),
            pltpu.VMEM((heads, width, rows), bf16),
            pltpu.VMEM((heads, 1, rows), f32),
            pltpu.VMEM((heads, width + 16, rows), f32),
            pltpu.VMEM((rows, rows), f32),
            pltpu.VMEM((rows, rows), f32),
            pltpu.VMEM((prompts,) + piece, bf16),
            pltpu.VMEM((prompts,) + piece, bf16),
            pltpu.VMEM((prompts,) + piece, bf16),
            pltpu.VMEM((rows, width), f32),
            dma((3, ROUNDS)),
            dma((3, ROUNDS)),
            dma((prompts,)),
            dma((prompts,)),
            dma((blocks,)),
            dma((blocks,)),
        ],
        compiler_params=pltpu.CompilerParams(
            collective_id=0, has_side_effects=True, vmem_limit_bytes=56 << 20
        ),
    )(
        spans,
        partner,
        queries.transpose(1, 0, 2),
        keys.transpose(1, 0, 2),
        values.transpose(1, 0, 2),
    )
    return attended.transpose(1, 0, 2), cache


def solution(mesh):
    placed = (
        P(("prompt", "ctx"), None, None),
        P(("prompt", "ctx"), None, None),
        P(("prompt", "ctx"), None, None),
        P("prompt", None),
        P(),
    )
    return jax.shard_map(
        per_device,
        mesh=mesh,
        in_specs=placed,
        out_specs=(P(("prompt", "ctx"), None, None), P("ctx", None, "prompt", None, None, None)),
        check_vma=False,
    )
```

```python
import functools
import math

import jax
import jax.numpy as jnp
from jax import lax
from jax.experimental import pallas as pl
from jax.experimental.pallas import tpu as pltpu
from jax.sharding import PartitionSpec as P

LOG2E = 1.4426950408889634
MESH = pl.DeviceIdType.MESH
ROUNDS = 10
CROSS = 8
HAND_ROUND = 5
LATE_ROUND = 8
DOT = (((1,), (0,)), ((), ()))


def fused_kernel(
    spans_ref, partner_ref, q_ref, k_ref, v_ref, o_ref, cache_ref,
    own, plain, raw, turned, inbox, qt, peak, acc, score_a, score_b, spread, gathered, chosen, via, wide,
    link_send, link_recv, spread_send, spread_recv, hand_send, hand_recv, via_send, via_recv, raw_sem,
):
    rows, heads, width = q_ref.shape
    groups = k_ref.shape[1]
    members = heads // groups
    tiles = rows // width
    scale = LOG2E / math.sqrt(width)
    scores = (score_a, score_b)

    prompts, blocks = lax.axis_size("prompt"), lax.axis_size("ctx")
    p, c = lax.axis_index("prompt"), lax.axis_index("ctx")
    ring = blocks // 2
    half, y = c // ring, c % ring
    ahead = (p, half * ring + (y + 1) % ring)
    behind = (p, half * ring + (y + ring - 1) % ring)
    across = (p, ring + y)
    length = spans_ref[0, 0] + spans_ref[0, 1]
    ahead_rounds = jnp.where(half == 0, 8, ROUNDS)
    behind_rounds = jnp.where(half == 0, 4, ROUNDS)

    barrier = pltpu.get_barrier_semaphore()

    def greet_prompt(k, carry):
        pl.semaphore_signal(barrier, inc=1, device_id=((p + k) % prompts, c), device_id_type=MESH)
        return carry

    def greet_ctx(k, carry):
        pl.semaphore_signal(barrier, inc=1, device_id=(p, (c + k) % blocks), device_id_type=MESH)
        return carry

    lax.fori_loop(1, prompts, greet_prompt, 0)
    lax.fori_loop(1, blocks, greet_ctx, 0)

    fetch = pltpu.make_async_copy(q_ref, raw, raw_sem)
    fetch.start()

    for t in range(tiles):
        part = slice(t * width, (t + 1) * width)
        by_head = jnp.swapaxes(k_ref[part], 0, 1)
        values_by_head = jnp.swapaxes(v_ref[part], 0, 1)
        for g in range(groups):
            own[g, part, :] = by_head[g]
            plain[g, part, :] = values_by_head[g]
            own[g, rows + t * width : rows + (t + 1) * width, :] = values_by_head[g].T
    pl.semaphore_wait(barrier, prompts + blocks - 2)

    def put(src, dst, lane, i, recv, target):
        return pltpu.make_async_remote_copy(
            src_ref=src, dst_ref=dst, send_sem=link_send.at[lane, i], recv_sem=recv,
            device_id=target, device_id_type=MESH,
        )

    def send_ahead(src, i):
        put(src, inbox.at[0, i], 0, i, link_recv.at[0, i], ahead).start()

    def send_behind(src, i):
        put(src, inbox.at[1, i], 1, i, link_recv.at[1, i], behind).start()

    def send_across(src, i):
        put(src, inbox.at[2, i + 1], 2, i, link_recv.at[2, i + 1], across).start()

    for i in range(groups):
        send_ahead(own.at[i], i)
        send_behind(own.at[i], i)

        @pl.when(half == 0)
        def _():
            send_across(own.at[i], i)

    fetch.wait()
    cut = 64

    def sort_heads(b, carry):
        first = pl.multiple_of(b * cut, cut)
        by_head = jnp.swapaxes(raw[pl.ds(first, cut)], 0, 1)
        for n in range(heads):
            turned[n, pl.ds(first, cut), :] = by_head[n]
        return carry

    lax.fori_loop(0, rows // cut, sort_heads, 0)

    def turn(n, carry):
        qt[n] = turned[n].T
        peak[n] = jnp.full((1, rows), -1e30, jnp.float32)
        acc[n] = jnp.zeros(acc.shape[1:], jnp.float32)
        return carry

    lax.fori_loop(0, heads, turn, 0)

    position = c * rows + lax.broadcasted_iota(jnp.int32, (rows, width), 0)
    stripes = spread.shape[0] // groups
    stripe_rows = rows // stripes
    for part, ref in enumerate((own, plain)):
        for g in range(groups):
            wide[...] = jnp.where(position < length, ref[g, 0:rows].astype(jnp.float32), 0.0)
            for st in range(stripes):
                spread[st * groups + g, part] = wide[pl.ds(st, stripe_rows, stride=stripes), :].astype(jnp.bfloat16)

    def spread_copy(s):
        return pltpu.make_async_remote_copy(
            src_ref=spread.at[s], dst_ref=gathered.at[p], send_sem=spread_send.at[s],
            recv_sem=spread_recv.at[p], device_id=(s, c), device_id_type=MESH,
        )

    def spread_start(k, carry):
        spread_copy((p + k) % prompts).start()
        return carry

    gathered[p] = spread[p]
    lax.fori_loop(1, prompts, spread_start, 0)

    def score(chunk, g, m):
        return lax.dot_general(
            chunk[0:rows, :], qt[g * members + m], DOT, preferred_element_type=jnp.float32
        )

    def fold(chunk, g, m, s, mask):
        n = g * members + m
        if mask is not None:
            s = jnp.where(mask, s, -1e30)
        before = peak[n]
        top = jnp.maximum(before, jnp.max(s, axis=0, keepdims=True))
        weight = jnp.exp2(s * scale - top * scale).astype(jnp.bfloat16)
        turned = jnp.concatenate(
            [chunk[rows + t * width : rows + (t + 1) * width, :] for t in range(tiles)], axis=1
        )
        turned = jnp.concatenate([turned, jnp.ones((acc.shape[1] - width, rows), jnp.bfloat16)], axis=0)
        mixed = lax.dot_general(turned, weight, DOT, preferred_element_type=jnp.float32)
        acc[n] = acc[n] * jnp.exp2((before - top) * scale) + mixed
        peak[n] = top

    def run(units, mask=None):
        chunk, g, m = units[0]
        scores[0][...] = score(chunk, g, m)
        for i, (chunk, g, m) in enumerate(units):
            if i + 1 < len(units):
                scores[(i + 1) % 2][...] = score(*units[i + 1])
            fold(chunk, g, m, scores[i % 2][...], mask)

    key_row = lax.broadcasted_iota(jnp.int32, (rows, rows), 0)
    query_row = lax.broadcasted_iota(jnp.int32, (rows, rows), 1)

    def diagonal(g, carry):
        mask = (key_row <= query_row) & ((c * rows + key_row < length) | (key_row == 0))
        run([(own.at[g], g, m) for m in range(members)], mask)
        return carry

    lax.fori_loop(0, groups, diagonal, 0)

    def lane_block(lane, i):
        near, far = half * ring, (1 - half) * ring
        ahead_block = jnp.where(
            i < 4, near + (y + ring - 1) % ring, jnp.where(i < 8, near + (y + 2) % ring, far + (y + 2) % ring)
        )
        behind_block = jnp.where(
            i < 4, near + (y + 1) % ring, jnp.where(i < 8, far + (y + 1) % ring, far + (y + 2) % ring)
        )
        across_block = jnp.where(i < 5, far + y, far + (y + ring - 1) % ring)
        block = jnp.where(lane == 0, ahead_block, jnp.where(lane == 1, behind_block, across_block))
        behind_head = jnp.where(i < 8, i % 4, i - 6)
        head = jnp.where(lane == 0, i % 4, jnp.where(lane == 1, behind_head, (i + 3) % 4))
        return block, head

    def arrived(lane, i):
        put(inbox.at[lane, i], inbox.at[lane, i], lane, i, link_recv.at[lane, i], ahead).wait_recv()

    def hand_copy(rows_of, sem, dst, recv, target):
        return pltpu.make_async_remote_copy(
            src_ref=chosen.at[pl.ds(2 * rows_of, 2)], dst_ref=dst, send_sem=hand_send.at[sem],
            recv_sem=recv, device_id=(p, target), device_id_type=MESH,
        )

    def hand_direct(target):
        hand_copy(target, target, cache_ref.at[:, :, 0, c], hand_recv.at[c], target).start()

    def forward_copy(source):
        return pltpu.make_async_remote_copy(
            src_ref=via.at[source], dst_ref=cache_ref.at[:, :, 0, source], send_sem=via_send.at[source],
            recv_sem=hand_recv.at[source], device_id=(p, ring + y), device_id_type=MESH,
        )

    def via_copy(beside):
        return hand_copy(ring + beside, ring + beside, via.at[y], via_recv.at[y], beside)

    def round_trip(i, carry):
        @pl.when(i < ahead_rounds)
        def _():
            arrived(0, i)

        @pl.when(i < 4)
        def _():
            send_ahead(inbox.at[0, i], i + 4)

            @pl.when(half == 0)
            def _():
                send_across(inbox.at[0, i], i + 4)

        @pl.when(i < behind_rounds)
        def _():
            arrived(1, i)

        @pl.when((half == 1) & (i >= 6) & (i < 8))
        def _():
            send_behind(inbox.at[1, i], i + 2)

        crossing = (half == 1) & (i >= 1) & (i <= CROSS)

        @pl.when(crossing)
        def _():
            arrived(2, i)

            @pl.when(i <= 4)
            def _():
                send_behind(inbox.at[2, i], i + 3)

            @pl.when((i >= 5) & (i <= 6))
            def _():
                send_ahead(inbox.at[2, i], i + 3)

        @pl.when(i == HAND_ROUND)
        def _():
            def collect(k, inner):
                source = (p + k) % prompts
                pltpu.make_async_remote_copy(
                    src_ref=spread.at[source], dst_ref=gathered.at[source], send_sem=spread_send.at[source],
                    recv_sem=spread_recv.at[source], device_id=(source, c), device_id_type=MESH,
                ).wait_recv()
                return inner

            lax.fori_loop(1, prompts, collect, 0)
            for b in range(chosen.shape[0]):
                chosen[b] = gathered[partner_ref[b]]
            cache_ref[:, :, 0, c] = chosen[pl.ds(2 * c, 2)]

            @pl.when(half == 0)
            def _():
                hand_direct(ring + y)

                def beside_start(k, inner):
                    via_copy((y + k) % ring).start()
                    hand_direct((y + k) % ring)
                    return inner

                lax.fori_loop(1, ring, beside_start, 0)

            @pl.when(half == 1)
            def _():
                def across_start(k, inner):
                    hand_direct((y + k) % ring)
                    return inner

                lax.fori_loop(0, ring, across_start, 0)

        @pl.when((i == LATE_ROUND) & (half == 1))
        def _():
            def near_start(k, inner):
                hand_direct(ring + (y + k) % ring)
                return inner

            lax.fori_loop(1, ring, near_start, 0)

        @pl.when((i == LATE_ROUND) & (half == 0))
        def _():
            def forward(k, inner):
                source = (y + k) % ring
                pltpu.make_async_remote_copy(
                    src_ref=via.at[source], dst_ref=via.at[source], send_sem=via_send.at[source],
                    recv_sem=via_recv.at[source], device_id=(p, source), device_id_type=MESH,
                ).wait_recv()
                forward_copy(source).start()
                return inner

            lax.fori_loop(1, ring, forward, 0)

        places = [lane_block(lane, i) for lane in range(3)]
        every = crossing & (places[0][0] < c) & (places[1][0] < c) & (places[2][0] < c)

        @pl.when(every)
        def _():
            run([(inbox.at[lane, i], places[lane][1], m) for lane in range(3) for m in range(members)])

        @pl.when(jnp.logical_not(every))
        def _():
            def one(lane, inner):
                block, g = lane_block(lane, i)

                @pl.when((block < c) & ((lane < 2) | crossing))
                def _():
                    run([(inbox.at[lane, i], g, m) for m in range(members)])

                return inner

            lax.fori_loop(0, 3, one, 0)

        return carry

    lax.fori_loop(0, ROUNDS, round_trip, 0)

    live = c * rows + lax.broadcasted_iota(jnp.int32, (rows, width), 0) < length

    def finish(n, carry):
        total = acc[n]
        mixture = (total[0:width] / total[width : width + 1]).T
        turned[n] = jnp.where(live, mixture, 0.0).astype(jnp.bfloat16)
        return carry

    lax.fori_loop(0, heads, finish, 0)

    def sort_rows(b, carry):
        first = pl.multiple_of(b * cut, cut)
        o_ref[pl.ds(first, cut)] = jnp.swapaxes(turned[:, pl.ds(first, cut), :], 0, 1)
        return carry

    lax.fori_loop(0, rows // cut, sort_rows, 0)

    def sent(i, carry):
        def left(lane, going):
            @pl.when(going)
            def _():
                put(inbox.at[0, i], inbox.at[0, i], lane, i, link_recv.at[0, i], ahead).wait_send()

        left(0, i < ahead_rounds)
        left(1, i < behind_rounds)
        left(2, (half == 0) & (i < CROSS))
        return carry

    lax.fori_loop(0, ROUNDS, sent, 0)

    def spread_done(k, carry):
        spread_copy((p + k) % prompts).wait_send()
        return carry

    lax.fori_loop(1, prompts, spread_done, 0)

    @pl.when(half == 0)
    def _():
        def forwarded(k, carry):
            forward_copy((y + k) % ring).wait_send()
            return carry

        lax.fori_loop(1, ring, forwarded, 0)

    def hand_done(k, carry):
        other = (c + k) % blocks
        done = hand_copy(other, other, cache_ref.at[:, :, 0, other], hand_recv.at[other], other)
        done.wait_send()
        done.wait_recv()
        return carry

    lax.fori_loop(1, blocks, hand_done, 0)


def per_device(queries, keys, values, spans, partner):
    rows, heads, width = queries.shape
    groups = keys.shape[1]
    prompts, blocks = lax.axis_size("prompt"), lax.axis_size("ctx")
    stripe_rows = rows * groups // prompts
    vmem, smem = pl.BlockSpec(memory_space=pltpu.VMEM), pl.BlockSpec(memory_space=pltpu.SMEM)
    bf16, f32, dma = jnp.bfloat16, jnp.float32, pltpu.SemaphoreType.DMA
    piece = (2, stripe_rows, width)
    return pl.pallas_call(
        fused_kernel,
        out_shape=(
            jax.ShapeDtypeStruct((rows, heads, width), bf16),
            jax.ShapeDtypeStruct((2, 2, 1, blocks, stripe_rows, width), bf16),
        ),
        in_specs=[smem, smem, pl.BlockSpec(memory_space=pl.ANY), vmem, vmem],
        out_specs=(vmem, vmem),
        scratch_shapes=[
            pltpu.VMEM((groups, 2 * rows, width), bf16),
            pltpu.VMEM((groups, rows, width), bf16),
            pltpu.VMEM((rows, heads, width), bf16),
            pltpu.VMEM((heads, rows, width), bf16),
            pltpu.VMEM((3, ROUNDS, 2 * rows, width), bf16),
            pltpu.VMEM((heads, width, rows), bf16),
            pltpu.VMEM((heads, 1, rows), f32),
            pltpu.VMEM((heads, width + 16, rows), f32),
            pltpu.VMEM((rows, rows), f32),
            pltpu.VMEM((rows, rows), f32),
            pltpu.VMEM((prompts,) + piece, bf16),
            pltpu.VMEM((prompts,) + piece, bf16),
            pltpu.VMEM((prompts,) + piece, bf16),
            pltpu.VMEM((blocks // 2, 2) + piece, bf16),
            pltpu.VMEM((rows, width), f32),
            dma((3, ROUNDS)),
            dma((3, ROUNDS)),
            dma((prompts,)),
            dma((prompts,)),
            dma((blocks,)),
            dma((blocks,)),
            dma((blocks // 2,)),
            dma((blocks // 2,)),
            dma,
        ],
        compiler_params=pltpu.CompilerParams(
            collective_id=0, has_side_effects=True, vmem_limit_bytes=56 << 20
        ),
    )(spans, partner, queries, keys, values)


def solution(mesh):
    placed = (
        P(("prompt", "ctx"), None, None),
        P(("prompt", "ctx"), None, None),
        P(("prompt", "ctx"), None, None),
        P("prompt", None),
        P(),
    )
    return jax.shard_map(
        per_device,
        mesh=mesh,
        in_specs=placed,
        out_specs=(P(("prompt", "ctx"), None, None), P("ctx", None, "prompt", None, None, None)),
        check_vma=False,
    )
```

```python
import functools
import math

import jax
import jax.numpy as jnp
from jax import lax
from jax.experimental import pallas as pl
from jax.experimental.pallas import tpu as pltpu
from jax.sharding import PartitionSpec as P

LOG2E = 1.4426950408889634
MESH = pl.DeviceIdType.MESH
ROUNDS = 10
CROSS = 8
HAND_ROUND = 5
LATE_ROUND = 8
DOT = (((1,), (0,)), ((), ()))


def fused_kernel(
    spans_ref, partner_ref, q_ref, k_ref, v_ref, o_ref, cache_ref,
    own, plain, raw, turned, inbox, qt, peak, acc, score_a, score_b, spread, gathered, chosen, via, wide,
    link_send, link_recv, spread_send, spread_recv, hand_send, hand_recv, via_send, via_recv, raw_sem, out_sem, word,
):
    rows, heads, width = q_ref.shape
    groups = k_ref.shape[1]
    members = heads // groups
    tiles = rows // width
    scale = LOG2E / math.sqrt(width)
    scores = (score_a, score_b)

    prompts, blocks = lax.axis_size("prompt"), lax.axis_size("ctx")
    p, c = lax.axis_index("prompt"), lax.axis_index("ctx")
    ring = blocks // 2
    half, y = c // ring, c % ring
    ahead = (p, half * ring + (y + 1) % ring)
    behind = (p, half * ring + (y + ring - 1) % ring)
    across = (p, ring + y)
    length = spans_ref[0, 0] + spans_ref[0, 1]
    ahead_rounds = jnp.where(half == 0, 8, ROUNDS)
    behind_rounds = jnp.where(half == 0, 4, ROUNDS)

    near = (
        ((p + 4) % prompts, c),
        ((p + prompts - 4) % prompts, c),
        (p + 2 - 4 * ((p // 2) % 2), c),
        (p + 1 - 2 * (p % 2), c),
        ahead,
        behind,
        (p, (1 - half) * ring + y),
    )
    barrier = pltpu.get_barrier_semaphore()
    for device in near:
        pl.semaphore_signal(barrier, inc=1, device_id=device, device_id_type=MESH)

    def pass_word(stage):
        for device in near[:4]:
            pl.semaphore_signal(word.at[stage], inc=1, device_id=device, device_id_type=MESH)

    def hear_word(stage):
        pl.semaphore_wait(word.at[stage], 4)

    fetch = pltpu.make_async_copy(q_ref, raw, raw_sem)
    fetch.start()

    for t in range(tiles):
        part = slice(t * width, (t + 1) * width)
        by_head = jnp.swapaxes(k_ref[part], 0, 1)
        values_by_head = jnp.swapaxes(v_ref[part], 0, 1)
        for g in range(groups):
            own[g, part, :] = by_head[g]
            plain[g, part, :] = values_by_head[g]
            own[g, rows + t * width : rows + (t + 1) * width, :] = values_by_head[g].T
    pl.semaphore_wait(barrier, len(near))
    pass_word(0)

    def put(src, dst, lane, i, recv, target):
        return pltpu.make_async_remote_copy(
            src_ref=src, dst_ref=dst, send_sem=link_send.at[lane, i], recv_sem=recv,
            device_id=target, device_id_type=MESH,
        )

    def send_ahead(src, i):
        put(src, inbox.at[0, i], 0, i, link_recv.at[0, i], ahead).start()

    def send_behind(src, i):
        put(src, inbox.at[1, i], 1, i, link_recv.at[1, i], behind).start()

    def send_across(src, i):
        put(src, inbox.at[2, i + 1], 2, i, link_recv.at[2, i + 1], across).start()

    for i in range(groups):
        send_ahead(own.at[i], i)
        send_behind(own.at[i], i)

        @pl.when(half == 0)
        def _():
            send_across(own.at[i], i)

    fetch.wait()
    hear_word(0)
    pass_word(1)
    cut = 64

    def sort_heads(b, carry):
        first = pl.multiple_of(b * cut, cut)
        by_head = jnp.swapaxes(raw[pl.ds(first, cut)], 0, 1)
        for n in range(heads):
            turned[n, pl.ds(first, cut), :] = by_head[n]
        return carry

    lax.fori_loop(0, rows // cut, sort_heads, 0)

    def turn(n, carry):
        qt[n] = turned[n].T
        peak[n] = jnp.full((1, rows), -1e30, jnp.float32)
        acc[n] = jnp.zeros(acc.shape[1:], jnp.float32)
        return carry

    hear_word(1)
    pass_word(2)
    lax.fori_loop(0, heads, turn, 0)

    position = c * rows + lax.broadcasted_iota(jnp.int32, (rows, width), 0)
    stripes = spread.shape[0] // groups
    stripe_rows = rows // stripes
    for part, ref in enumerate((own, plain)):
        for g in range(groups):
            wide[...] = jnp.where(position < length, ref[g, 0:rows].astype(jnp.float32), 0.0)
            for st in range(stripes):
                spread[st * groups + g, part] = wide[pl.ds(st, stripe_rows, stride=stripes), :].astype(jnp.bfloat16)

    def spread_copy(s):
        return pltpu.make_async_remote_copy(
            src_ref=spread.at[s], dst_ref=gathered.at[p], send_sem=spread_send.at[s],
            recv_sem=spread_recv.at[p], device_id=(s, c), device_id_type=MESH,
        )

    def spread_start(k, carry):
        spread_copy((p + k) % prompts).start()
        return carry

    gathered[p] = spread[p]
    hear_word(2)
    lax.fori_loop(1, prompts, spread_start, 0)

    def score(chunk, g, m):
        return lax.dot_general(
            chunk[0:rows, :], qt[g * members + m], DOT, preferred_element_type=jnp.float32
        )

    def fold(chunk, g, m, s, mask):
        n = g * members + m
        if mask is not None:
            s = jnp.where(mask, s, -1e30)
        before = peak[n]
        top = jnp.maximum(before, jnp.max(s, axis=0, keepdims=True))
        weight = jnp.exp2(s * scale - top * scale).astype(jnp.bfloat16)
        turned = jnp.concatenate(
            [chunk[rows + t * width : rows + (t + 1) * width, :] for t in range(tiles)], axis=1
        )
        turned = jnp.concatenate([turned, jnp.ones((acc.shape[1] - width, rows), jnp.bfloat16)], axis=0)
        mixed = lax.dot_general(turned, weight, DOT, preferred_element_type=jnp.float32)
        acc[n] = acc[n] * jnp.exp2((before - top) * scale) + mixed
        peak[n] = top

    def run(units, mask=None):
        chunk, g, m = units[0]
        scores[0][...] = score(chunk, g, m)
        for i, (chunk, g, m) in enumerate(units):
            if i + 1 < len(units):
                scores[(i + 1) % 2][...] = score(*units[i + 1])
            fold(chunk, g, m, scores[i % 2][...], mask)

    key_row = lax.broadcasted_iota(jnp.int32, (rows, rows), 0)
    query_row = lax.broadcasted_iota(jnp.int32, (rows, rows), 1)

    def diagonal(g, carry):
        mask = (key_row <= query_row) & ((c * rows + key_row < length) | (key_row == 0))
        run([(own.at[g], g, m) for m in range(members)], mask)
        return carry

    lax.fori_loop(0, groups, diagonal, 0)

    def lane_block(lane, i):
        near, far = half * ring, (1 - half) * ring
        ahead_block = jnp.where(
            i < 4, near + (y + ring - 1) % ring, jnp.where(i < 8, near + (y + 2) % ring, far + (y + 2) % ring)
        )
        behind_block = jnp.where(
            i < 4, near + (y + 1) % ring, jnp.where(i < 8, far + (y + 1) % ring, far + (y + 2) % ring)
        )
        across_block = jnp.where(i < 5, far + y, far + (y + ring - 1) % ring)
        block = jnp.where(lane == 0, ahead_block, jnp.where(lane == 1, behind_block, across_block))
        behind_head = jnp.where(i < 8, i % 4, i - 6)
        head = jnp.where(lane == 0, i % 4, jnp.where(lane == 1, behind_head, (i + 3) % 4))
        return block, head

    def arrived(lane, i):
        put(inbox.at[lane, i], inbox.at[lane, i], lane, i, link_recv.at[lane, i], ahead).wait_recv()

    def hand_copy(rows_of, sem, dst, recv, target):
        return pltpu.make_async_remote_copy(
            src_ref=chosen.at[pl.ds(2 * rows_of, 2)], dst_ref=dst, send_sem=hand_send.at[sem],
            recv_sem=recv, device_id=(p, target), device_id_type=MESH,
        )

    def hand_direct(target):
        hand_copy(target, target, cache_ref.at[:, :, 0, c], hand_recv.at[c], target).start()

    def forward_copy(source):
        return pltpu.make_async_remote_copy(
            src_ref=via.at[source], dst_ref=cache_ref.at[:, :, 0, source], send_sem=via_send.at[source],
            recv_sem=hand_recv.at[source], device_id=(p, ring + y), device_id_type=MESH,
        )

    def via_copy(beside):
        return hand_copy(ring + beside, ring + beside, via.at[y], via_recv.at[y], beside)

    live = c * rows + lax.broadcasted_iota(jnp.int32, (width, rows), 1) < length

    def finish(n):
        total = acc[n]
        mixture = total[0:width] * (1.0 / total[width : width + 1])
        turned[n] = jnp.where(live, mixture, 0.0).astype(jnp.bfloat16).T

    def early_head(k):
        return (k // members) * 2 * members + k % members

    def round_trip(i, carry):
        @pl.when(i == ROUNDS - 1)
        def _():
            def early_finish(k, inner):
                finish(early_head(k))
                return inner

            lax.fori_loop(0, heads // 2, early_finish, 0)

        @pl.when(i < ahead_rounds)
        def _():
            arrived(0, i)

        @pl.when(i < 4)
        def _():
            send_ahead(inbox.at[0, i], i + 4)

            @pl.when(half == 0)
            def _():
                send_across(inbox.at[0, i], i + 4)

        @pl.when(i < behind_rounds)
        def _():
            arrived(1, i)

        @pl.when((half == 1) & (i >= 6) & (i < 8))
        def _():
            send_behind(inbox.at[1, i], i + 2)

        crossing = (half == 1) & (i >= 1) & (i <= CROSS)

        @pl.when(crossing)
        def _():
            arrived(2, i)

            @pl.when(i <= 4)
            def _():
                send_behind(inbox.at[2, i], i + 3)

            @pl.when((i >= 5) & (i <= 6))
            def _():
                send_ahead(inbox.at[2, i], i + 3)

        @pl.when(i == HAND_ROUND)
        def _():
            def collect(k, inner):
                source = (p + k) % prompts
                pltpu.make_async_remote_copy(
                    src_ref=spread.at[source], dst_ref=gathered.at[source], send_sem=spread_send.at[source],
                    recv_sem=spread_recv.at[source], device_id=(source, c), device_id_type=MESH,
                ).wait_recv()
                return inner

            lax.fori_loop(1, prompts, collect, 0)
            for b in range(chosen.shape[0]):
                chosen[b] = gathered[partner_ref[b]]
            cache_ref[:, :, 0, c] = chosen[pl.ds(2 * c, 2)]

            @pl.when(half == 0)
            def _():
                hand_direct(ring + y)

                def beside_start(k, inner):
                    via_copy((y + k) % ring).start()
                    hand_direct((y + k) % ring)
                    return inner

                lax.fori_loop(1, ring, beside_start, 0)

            @pl.when(half == 1)
            def _():
                def across_start(k, inner):
                    hand_direct((y + k) % ring)
                    return inner

                lax.fori_loop(0, ring, across_start, 0)

        @pl.when((i == LATE_ROUND) & (half == 1))
        def _():
            def near_start(k, inner):
                hand_direct(ring + (y + k) % ring)
                return inner

            lax.fori_loop(1, ring, near_start, 0)

        @pl.when((i == LATE_ROUND) & (half == 0))
        def _():
            def forward(k, inner):
                source = (y + k) % ring
                pltpu.make_async_remote_copy(
                    src_ref=via.at[source], dst_ref=via.at[source], send_sem=via_send.at[source],
                    recv_sem=via_recv.at[source], device_id=(p, source), device_id_type=MESH,
                ).wait_recv()
                forward_copy(source).start()
                return inner

            lax.fori_loop(1, ring, forward, 0)

        places = [lane_block(lane, i) for lane in range(3)]
        every = crossing & (places[0][0] < c) & (places[1][0] < c) & (places[2][0] < c)

        @pl.when(every)
        def _():
            run([(inbox.at[lane, i], places[lane][1], m) for lane in range(3) for m in range(members)])

        @pl.when(jnp.logical_not(every))
        def _():
            def one(lane, inner):
                block, g = lane_block(lane, i)

                @pl.when((block < c) & ((lane < 2) | crossing))
                def _():
                    run([(inbox.at[lane, i], g, m) for m in range(members)])

                return inner

            lax.fori_loop(0, 3, one, 0)

        return carry

    lax.fori_loop(0, ROUNDS, round_trip, 0)

    def leave(n):
        return pltpu.make_async_copy(turned.at[n], o_ref.at[n], out_sem.at[n])

    def early_leave(k, carry):
        leave(early_head(k)).start()
        return carry

    lax.fori_loop(0, heads // 2, early_leave, 0)

    def late_finish(k, carry):
        finish(early_head(k) + members)

        @pl.when(k > 0)
        def _():
            leave(early_head(k - 1) + members).start()

        return carry

    lax.fori_loop(0, heads // 2, late_finish, 0)

    def sent(i, carry):
        def left(lane, going):
            @pl.when(going)
            def _():
                put(inbox.at[0, i], inbox.at[0, i], lane, i, link_recv.at[0, i], ahead).wait_send()

        left(0, i < ahead_rounds)
        left(1, i < behind_rounds)
        left(2, (half == 0) & (i < CROSS))
        return carry

    lax.fori_loop(0, ROUNDS, sent, 0)
    leave(heads - 1).start()

    def left_for_good(n, carry):
        leave(n).wait()
        return carry

    lax.fori_loop(0, heads, left_for_good, 0)

    def spread_done(k, carry):
        spread_copy((p + k) % prompts).wait_send()
        return carry

    lax.fori_loop(1, prompts, spread_done, 0)

    @pl.when(half == 0)
    def _():
        def forwarded(k, carry):
            forward_copy((y + k) % ring).wait_send()
            return carry

        lax.fori_loop(1, ring, forwarded, 0)

    def hand_done(k, carry):
        other = (c + k) % blocks
        done = hand_copy(other, other, cache_ref.at[:, :, 0, other], hand_recv.at[other], other)
        done.wait_send()
        done.wait_recv()
        return carry

    lax.fori_loop(1, blocks, hand_done, 0)


def place_kernel(head_ref, cache_in, o_ref, cache_out):
    o_ref[...] = jnp.swapaxes(head_ref[...], 0, 1)
    cache_out[...] = cache_in[...]


def per_device(queries, keys, values, spans, partner):
    rows, heads, width = queries.shape
    groups = keys.shape[1]
    prompts, blocks = lax.axis_size("prompt"), lax.axis_size("ctx")
    stripe_rows = rows * groups // prompts
    vmem, smem = pl.BlockSpec(memory_space=pltpu.VMEM), pl.BlockSpec(memory_space=pltpu.SMEM)
    bf16, f32, dma = jnp.bfloat16, jnp.float32, pltpu.SemaphoreType.DMA
    piece = (2, stripe_rows, width)
    by_head, cache = pl.pallas_call(
        fused_kernel,
        out_shape=(
            jax.ShapeDtypeStruct((heads, rows, width), bf16),
            jax.ShapeDtypeStruct((2, 2, 1, blocks, stripe_rows, width), bf16),
        ),
        in_specs=[smem, smem, pl.BlockSpec(memory_space=pl.ANY), vmem, vmem],
        out_specs=(pl.BlockSpec(memory_space=pl.ANY), vmem),
        scratch_shapes=[
            pltpu.VMEM((groups, 2 * rows, width), bf16),
            pltpu.VMEM((groups, rows, width), bf16),
            pltpu.VMEM((rows, heads, width), bf16),
            pltpu.VMEM((heads, rows, width), bf16),
            pltpu.VMEM((3, ROUNDS, 2 * rows, width), bf16),
            pltpu.VMEM((heads, width, rows), bf16),
            pltpu.VMEM((heads, 1, rows), f32),
            pltpu.VMEM((heads, width + 16, rows), f32),
            pltpu.VMEM((rows, rows), f32),
            pltpu.VMEM((rows, rows), f32),
            pltpu.VMEM((prompts,) + piece, bf16),
            pltpu.VMEM((prompts,) + piece, bf16),
            pltpu.VMEM((prompts,) + piece, bf16),
            pltpu.VMEM((blocks // 2, 2) + piece, bf16),
            pltpu.VMEM((rows, width), f32),
            dma((3, ROUNDS)),
            dma((3, ROUNDS)),
            dma((prompts,)),
            dma((prompts,)),
            dma((blocks,)),
            dma((blocks,)),
            dma((blocks // 2,)),
            dma((blocks // 2,)),
            dma,
            dma((heads,)),
            pltpu.SemaphoreType.REGULAR((3,)),
        ],
        compiler_params=pltpu.CompilerParams(
            collective_id=0, has_side_effects=True, vmem_limit_bytes=56 << 20
        ),
    )(spans, partner, queries, keys, values)
    steps = blocks // 4
    cache_block = pl.BlockSpec((2, 2, 1, 4, stripe_rows, width), lambda i: (0, 0, 0, i, 0, 0))
    return pl.pallas_call(
        place_kernel,
        out_shape=(jax.ShapeDtypeStruct(queries.shape, bf16), jax.ShapeDtypeStruct(cache.shape, bf16)),
        grid=(steps,),
        in_specs=[pl.BlockSpec((heads, rows // steps, width), lambda i: (0, i, 0)), cache_block],
        out_specs=(pl.BlockSpec((rows // steps, heads, width), lambda i: (i, 0, 0)), cache_block),
        compiler_params=pltpu.CompilerParams(dimension_semantics=("arbitrary",)),
    )(by_head, cache)


def solution(mesh):
    placed = (
        P(("prompt", "ctx"), None, None),
        P(("prompt", "ctx"), None, None),
        P(("prompt", "ctx"), None, None),
        P("prompt", None),
        P(),
    )
    return jax.shard_map(
        per_device,
        mesh=mesh,
        in_specs=placed,
        out_specs=(P(("prompt", "ctx"), None, None), P("ctx", None, "prompt", None, None, None)),
        check_vma=False,
    )
```

```python
import functools
import math

import jax
import jax.numpy as jnp
from jax import lax
from jax.experimental import pallas as pl
from jax.experimental.pallas import tpu as pltpu
from jax.sharding import PartitionSpec as P

LOG2E = 1.4426950408889634
MESH = pl.DeviceIdType.MESH
ROUNDS = 10
CROSS = 8
HAND_ROUND = 5
LATE_ROUND = 8
DOT = (((1,), (0,)), ((), ()))


def fused_kernel(
    spans_ref, partner_ref, q_ref, k_ref, v_ref, o_ref, cache_ref,
    own, plain, raw, turned, inbox, qt, peak, acc, score_a, score_b, spread, gathered, chosen, via, wide,
    link_send, link_recv, spread_send, spread_recv, hand_send, hand_recv, via_send, via_recv, raw_sem, out_sem, word,
):
    rows, heads, width = q_ref.shape
    groups = k_ref.shape[1]
    members = heads // groups
    tiles = rows // width
    scale = LOG2E / math.sqrt(width)
    scores = (score_a, score_b)

    prompts, blocks = lax.axis_size("prompt"), lax.axis_size("ctx")
    p, c = lax.axis_index("prompt"), lax.axis_index("ctx")
    ring = blocks // 2
    half, y = c // ring, c % ring
    ahead = (p, half * ring + (y + 1) % ring)
    behind = (p, half * ring + (y + ring - 1) % ring)
    across = (p, ring + y)
    length = spans_ref[0, 0] + spans_ref[0, 1]
    ahead_rounds = jnp.where(half == 0, 6, ROUNDS)
    behind_rounds = jnp.where(half == 0, 6, ROUNDS)

    near = (
        ((p + 4) % prompts, c),
        ((p + prompts - 4) % prompts, c),
        (p + 2 - 4 * ((p // 2) % 2), c),
        (p + 1 - 2 * (p % 2), c),
        ahead,
        behind,
        (p, (1 - half) * ring + y),
    )
    barrier = pltpu.get_barrier_semaphore()
    for device in near:
        pl.semaphore_signal(barrier, inc=1, device_id=device, device_id_type=MESH)

    def pass_word(stage):
        for device in near[:4]:
            pl.semaphore_signal(word.at[stage], inc=1, device_id=device, device_id_type=MESH)

    def hear_word(stage):
        pl.semaphore_wait(word.at[stage], 4)

    fetch = pltpu.make_async_copy(q_ref, raw, raw_sem)
    fetch.start()

    for t in range(tiles):
        part = slice(t * width, (t + 1) * width)
        by_head = jnp.swapaxes(k_ref[part], 0, 1)
        values_by_head = jnp.swapaxes(v_ref[part], 0, 1)
        for g in range(groups):
            own[g, part, :] = by_head[g]
            plain[g, part, :] = values_by_head[g]
            own[g, rows + t * width : rows + (t + 1) * width, :] = values_by_head[g].T
    pl.semaphore_wait(barrier, len(near))
    pass_word(0)

    def put(src, dst, lane, i, recv, target):
        return pltpu.make_async_remote_copy(
            src_ref=src, dst_ref=dst, send_sem=link_send.at[lane, i], recv_sem=recv,
            device_id=target, device_id_type=MESH,
        )

    def send_ahead(src, i):
        put(src, inbox.at[0, i], 0, i, link_recv.at[0, i], ahead).start()

    def send_behind(src, i):
        put(src, inbox.at[1, i], 1, i, link_recv.at[1, i], behind).start()

    def send_across(src, i):
        put(src, inbox.at[2, i + 1], 2, i, link_recv.at[2, i + 1], across).start()

    for i in range(groups):
        send_ahead(own.at[i], i)
        send_behind(own.at[i], i)

        @pl.when(half == 0)
        def _():
            send_across(own.at[i], i)

    fetch.wait()
    hear_word(0)
    pass_word(1)
    cut = 64

    def sort_heads(b, carry):
        first = pl.multiple_of(b * cut, cut)
        by_head = jnp.swapaxes(raw[pl.ds(first, cut)], 0, 1)
        for n in range(heads):
            turned[n, pl.ds(first, cut), :] = by_head[n]
        return carry

    lax.fori_loop(0, rows // cut, sort_heads, 0)

    def turn(n, carry):
        qt[n] = turned[n].T
        peak[n] = jnp.full((1, rows), -1e30, jnp.float32)
        acc[n] = jnp.zeros(acc.shape[1:], jnp.float32)
        return carry

    hear_word(1)
    pass_word(2)
    lax.fori_loop(0, heads, turn, 0)

    position = c * rows + lax.broadcasted_iota(jnp.int32, (rows, width), 0)
    stripes = spread.shape[0] // groups
    stripe_rows = rows // stripes
    for part, ref in enumerate((own, plain)):
        for g in range(groups):
            wide[...] = jnp.where(position < length, ref[g, 0:rows].astype(jnp.float32), 0.0)
            for st in range(stripes):
                spread[st * groups + g, part] = wide[pl.ds(st, stripe_rows, stride=stripes), :].astype(jnp.bfloat16)

    def spread_copy(s):
        return pltpu.make_async_remote_copy(
            src_ref=spread.at[s], dst_ref=gathered.at[p], send_sem=spread_send.at[s],
            recv_sem=spread_recv.at[p], device_id=(s, c), device_id_type=MESH,
        )

    def spread_start(k, carry):
        spread_copy((p + k) % prompts).start()
        return carry

    gathered[p] = spread[p]
    hear_word(2)
    lax.fori_loop(1, prompts, spread_start, 0)

    def score(chunk, g, m):
        return lax.dot_general(
            chunk[0:rows, :], qt[g * members + m], DOT, preferred_element_type=jnp.float32
        )

    def fold(chunk, g, m, s, mask):
        n = g * members + m
        if mask is not None:
            s = jnp.where(mask, s, -1e30)
        before = peak[n]
        top = jnp.maximum(before, jnp.max(s, axis=0, keepdims=True))
        weight = jnp.exp2(s * scale - top * scale).astype(jnp.bfloat16)
        turned = jnp.concatenate(
            [chunk[rows + t * width : rows + (t + 1) * width, :] for t in range(tiles)], axis=1
        )
        turned = jnp.concatenate([turned, jnp.ones((acc.shape[1] - width, rows), jnp.bfloat16)], axis=0)
        mixed = lax.dot_general(turned, weight, DOT, preferred_element_type=jnp.float32)
        acc[n] = acc[n] * jnp.exp2((before - top) * scale) + mixed
        peak[n] = top

    def run(units, mask=None):
        chunk, g, m = units[0]
        scores[0][...] = score(chunk, g, m)
        for i, (chunk, g, m) in enumerate(units):
            if i + 1 < len(units):
                scores[(i + 1) % 2][...] = score(*units[i + 1])
            fold(chunk, g, m, scores[i % 2][...], mask)

    key_row = lax.broadcasted_iota(jnp.int32, (rows, rows), 0)
    query_row = lax.broadcasted_iota(jnp.int32, (rows, rows), 1)

    def diagonal(g, carry):
        mask = (key_row <= query_row) & ((c * rows + key_row < length) | (key_row == 0))
        run([(own.at[g], g, m) for m in range(members)], mask)
        return carry

    lax.fori_loop(0, groups, diagonal, 0)

    def lane_block(lane, i):
        near, far = half * ring, (1 - half) * ring
        ahead_block = jnp.where(
            i < 4, near + (y + ring - 1) % ring, jnp.where(i < 8, near + (y + 2) % ring, far + (y + 2) % ring)
        )
        behind_block = jnp.where(
            i < 4, near + (y + 1) % ring, jnp.where(i < 8, far + (y + 1) % ring, far + (y + 2) % ring)
        )
        split = (half == 0) & (i >= 4)
        behind_block = jnp.where(split, near + (y + 2) % ring, behind_block)
        across_block = jnp.where(i < 5, far + y, far + (y + ring - 1) % ring)
        block = jnp.where(lane == 0, ahead_block, jnp.where(lane == 1, behind_block, across_block))
        behind_head = jnp.where(split, (i - 2) % 4, jnp.where(i < 8, i % 4, (i - 6) % 4))
        head = jnp.where(lane == 0, i % 4, jnp.where(lane == 1, behind_head, (i + 3) % 4))
        return block, head

    def arrived(lane, i):
        put(inbox.at[lane, i], inbox.at[lane, i], lane, i, link_recv.at[lane, i], ahead).wait_recv()

    def hand_copy(rows_of, sem, dst, recv, target):
        return pltpu.make_async_remote_copy(
            src_ref=chosen.at[pl.ds(2 * rows_of, 2)], dst_ref=dst, send_sem=hand_send.at[sem],
            recv_sem=recv, device_id=(p, target), device_id_type=MESH,
        )

    def hand_direct(target):
        hand_copy(target, target, cache_ref.at[:, :, 0, c], hand_recv.at[c], target).start()

    def forward_copy(source):
        return pltpu.make_async_remote_copy(
            src_ref=via.at[source], dst_ref=cache_ref.at[:, :, 0, source], send_sem=via_send.at[source],
            recv_sem=hand_recv.at[source], device_id=(p, ring + y), device_id_type=MESH,
        )

    def via_copy(beside):
        return hand_copy(ring + beside, ring + beside, via.at[y], via_recv.at[y], beside)

    live = c * rows + lax.broadcasted_iota(jnp.int32, (width, rows), 1) < length

    def finish(n):
        total = acc[n]
        mixture = total[0:width] * (1.0 / total[width : width + 1])
        turned[n] = jnp.where(live, mixture, 0.0).astype(jnp.bfloat16).T

    def early_head(k):
        return (k // members) * 2 * members + k % members

    def round_trip(i, carry):
        @pl.when(i == ROUNDS - 1)
        def _():
            def early_finish(k, inner):
                finish(early_head(k))
                return inner

            lax.fori_loop(0, heads // 2, early_finish, 0)

        @pl.when(i < ahead_rounds)
        def _():
            arrived(0, i)

        @pl.when(i < jnp.where(half == 0, 2, 4))
        def _():
            send_ahead(inbox.at[0, i], i + 4)

        @pl.when((half == 0) & (i < 4))
        def _():
            send_across(inbox.at[0, i], i + 4)

        @pl.when(i < behind_rounds)
        def _():
            arrived(1, i)

        @pl.when((i >= behind_rounds - 4) & (i < behind_rounds - 2))
        def _():
            send_behind(inbox.at[1, i], i + 2)

        crossing = (half == 1) & (i >= 1) & (i <= CROSS)

        @pl.when(crossing)
        def _():
            arrived(2, i)

            @pl.when(i <= 4)
            def _():
                send_behind(inbox.at[2, i], i + 3)

            @pl.when((i >= 5) & (i <= 6))
            def _():
                send_ahead(inbox.at[2, i], i + 3)

        @pl.when(i == HAND_ROUND)
        def _():
            def collect(k, inner):
                source = (p + k) % prompts
                pltpu.make_async_remote_copy(
                    src_ref=spread.at[source], dst_ref=gathered.at[source], send_sem=spread_send.at[source],
                    recv_sem=spread_recv.at[source], device_id=(source, c), device_id_type=MESH,
                ).wait_recv()
                return inner

            lax.fori_loop(1, prompts, collect, 0)
            for b in range(chosen.shape[0]):
                chosen[b] = gathered[partner_ref[b]]
            cache_ref[:, :, 0, c] = chosen[pl.ds(2 * c, 2)]

            @pl.when(half == 0)
            def _():
                hand_direct(ring + y)

                def beside_start(k, inner):
                    via_copy((y + k) % ring).start()
                    hand_direct((y + k) % ring)
                    return inner

                lax.fori_loop(1, ring, beside_start, 0)

            @pl.when(half == 1)
            def _():
                def across_start(k, inner):
                    hand_direct((y + k) % ring)
                    return inner

                lax.fori_loop(0, ring, across_start, 0)

        @pl.when((i == LATE_ROUND) & (half == 1))
        def _():
            def near_start(k, inner):
                hand_direct(ring + (y + k) % ring)
                return inner

            lax.fori_loop(1, ring, near_start, 0)

        @pl.when((i == LATE_ROUND - 2) & (half == 0))
        def _():
            def forward(k, inner):
                source = (y + k) % ring
                pltpu.make_async_remote_copy(
                    src_ref=via.at[source], dst_ref=via.at[source], send_sem=via_send.at[source],
                    recv_sem=via_recv.at[source], device_id=(p, source), device_id_type=MESH,
                ).wait_recv()
                forward_copy(source).start()
                return inner

            lax.fori_loop(1, ring, forward, 0)

        places = [lane_block(lane, i) for lane in range(3)]
        every = crossing & (places[0][0] < c) & (places[1][0] < c) & (places[2][0] < c)

        @pl.when(every)
        def _():
            run([(inbox.at[lane, i], places[lane][1], m) for lane in range(3) for m in range(members)])

        last = (half == 1) & (i == ROUNDS - 1)

        @pl.when(last)
        def _():
            run([(inbox.at[lane, i], places[lane][1], m) for lane in range(2) for m in range(members)])

        @pl.when(jnp.logical_not(every | last))
        def _():
            def one(lane, inner):
                block, g = lane_block(lane, i)

                @pl.when((block < c) & (i < ahead_rounds) & ((lane < 2) | crossing))
                def _():
                    run([(inbox.at[lane, i], g, m) for m in range(members)])

                return inner

            lax.fori_loop(0, 3, one, 0)

        return carry

    lax.fori_loop(0, ROUNDS, round_trip, 0)

    def leave(n):
        return pltpu.make_async_copy(turned.at[n], o_ref.at[n], out_sem.at[n])

    def early_leave(k, carry):
        leave(early_head(k)).start()
        return carry

    lax.fori_loop(0, heads // 2, early_leave, 0)

    def late_finish(k, carry):
        finish(early_head(k) + members)

        @pl.when(k > 0)
        def _():
            leave(early_head(k - 1) + members).start()

        return carry

    lax.fori_loop(0, heads // 2, late_finish, 0)

    def sent(i, carry):
        def left(lane, going):
            @pl.when(going)
            def _():
                put(inbox.at[0, i], inbox.at[0, i], lane, i, link_recv.at[0, i], ahead).wait_send()

        left(0, i < ahead_rounds)
        left(1, i < behind_rounds)
        left(2, (half == 0) & (i < CROSS))
        return carry

    lax.fori_loop(0, ROUNDS, sent, 0)
    leave(heads - 1).start()

    def left_for_good(n, carry):
        leave(n).wait()
        return carry

    lax.fori_loop(0, heads, left_for_good, 0)

    def spread_done(k, carry):
        spread_copy((p + k) % prompts).wait_send()
        return carry

    lax.fori_loop(1, prompts, spread_done, 0)

    @pl.when(half == 0)
    def _():
        def forwarded(k, carry):
            forward_copy((y + k) % ring).wait_send()
            return carry

        lax.fori_loop(1, ring, forwarded, 0)

    def hand_done(k, carry):
        other = (c + k) % blocks
        done = hand_copy(other, other, cache_ref.at[:, :, 0, other], hand_recv.at[other], other)
        done.wait_send()
        done.wait_recv()
        return carry

    lax.fori_loop(1, blocks, hand_done, 0)


def place_kernel(head_ref, cache_in, o_ref, cache_out):
    o_ref[...] = jnp.swapaxes(head_ref[...], 0, 1)
    cache_out[...] = cache_in[...]


def per_device(queries, keys, values, spans, partner):
    rows, heads, width = queries.shape
    groups = keys.shape[1]
    prompts, blocks = lax.axis_size("prompt"), lax.axis_size("ctx")
    stripe_rows = rows * groups // prompts
    vmem, smem = pl.BlockSpec(memory_space=pltpu.VMEM), pl.BlockSpec(memory_space=pltpu.SMEM)
    bf16, f32, dma = jnp.bfloat16, jnp.float32, pltpu.SemaphoreType.DMA
    piece = (2, stripe_rows, width)
    by_head, cache = pl.pallas_call(
        fused_kernel,
        out_shape=(
            jax.ShapeDtypeStruct((heads, rows, width), bf16),
            jax.ShapeDtypeStruct((2, 2, 1, blocks, stripe_rows, width), bf16),
        ),
        in_specs=[smem, smem, pl.BlockSpec(memory_space=pl.ANY), vmem, vmem],
        out_specs=(pl.BlockSpec(memory_space=pl.ANY), vmem),
        scratch_shapes=[
            pltpu.VMEM((groups, 2 * rows, width), bf16),
            pltpu.VMEM((groups, rows, width), bf16),
            pltpu.VMEM((rows, heads, width), bf16),
            pltpu.VMEM((heads, rows, width), bf16),
            pltpu.VMEM((3, ROUNDS, 2 * rows, width), bf16),
            pltpu.VMEM((heads, width, rows), bf16),
            pltpu.VMEM((heads, 1, rows), f32),
            pltpu.VMEM((heads, width + 16, rows), f32),
            pltpu.VMEM((rows, rows), f32),
            pltpu.VMEM((rows, rows), f32),
            pltpu.VMEM((prompts,) + piece, bf16),
            pltpu.VMEM((prompts,) + piece, bf16),
            pltpu.VMEM((prompts,) + piece, bf16),
            pltpu.VMEM((blocks // 2, 2) + piece, bf16),
            pltpu.VMEM((rows, width), f32),
            dma((3, ROUNDS)),
            dma((3, ROUNDS)),
            dma((prompts,)),
            dma((prompts,)),
            dma((blocks,)),
            dma((blocks,)),
            dma((blocks // 2,)),
            dma((blocks // 2,)),
            dma,
            dma((heads,)),
            pltpu.SemaphoreType.REGULAR((3,)),
        ],
        compiler_params=pltpu.CompilerParams(
            collective_id=0, has_side_effects=True, vmem_limit_bytes=56 << 20
        ),
    )(spans, partner, queries, keys, values)
    steps = blocks // 4
    cache_block = pl.BlockSpec((2, 2, 1, 4, stripe_rows, width), lambda i: (0, 0, 0, i, 0, 0))
    return pl.pallas_call(
        place_kernel,
        out_shape=(jax.ShapeDtypeStruct(queries.shape, bf16), jax.ShapeDtypeStruct(cache.shape, bf16)),
        grid=(steps,),
        in_specs=[pl.BlockSpec((heads, rows // steps, width), lambda i: (0, i, 0)), cache_block],
        out_specs=(pl.BlockSpec((rows // steps, heads, width), lambda i: (i, 0, 0)), cache_block),
        compiler_params=pltpu.CompilerParams(dimension_semantics=("arbitrary",)),
    )(by_head, cache)


def solution(mesh):
    placed = (
        P(("prompt", "ctx"), None, None),
        P(("prompt", "ctx"), None, None),
        P(("prompt", "ctx"), None, None),
        P("prompt", None),
        P(),
    )
    return jax.shard_map(
        per_device,
        mesh=mesh,
        in_specs=placed,
        out_specs=(P(("prompt", "ctx"), None, None), P("ctx", None, "prompt", None, None, None)),
        check_vma=False,
    )
```
